32 devices in a mesh: tm: 32 (over z, y, x, core).
Axes of the slice: x: 2, y: 2, z: 4, core: 2. Of those that a mesh axis runs over, the one named last changes fastest.
Arguments:
- samples: int32 [65536, 128], P('tm'), may hold values from -8 to 7
Outputs:
- spectra: float32 [2, 128, 16384], P(None, None, 'tm')
The draws below stay inside these ranges and needn't reach their ends.
All inputs are finite; a program needn't handle non-finite values.
Results may differ from the reference program's by a relative error of at most 0.0003.
Values may be sent and summed in bfloat16 or wider, within the bound.
No kernel may reach another device: no remote copies, remote signals or barrier semaphores. Data moves between devices by JAX's collectives and lax.ppermute only.
A program may use at most 192 MiB of HBM per device.

```python
import jax
import jax.numpy as jnp
from jax import lax

INPUTS = 128
LAGS = 128
TOTAL = 65536


def plant(drawn, stream_key, least, high):
    shape = drawn.shape
    index_at = [jax.random.randint(jax.random.fold_in(stream_key, axis), (), 0, shape[axis]) for axis in range(len(shape))]
    drawn = drawn.at[tuple(index_at)].set(least)
    longest = shape.index(max(shape))
    index_at[longest] = (index_at[longest] + 1) % shape[longest]
    return drawn.at[tuple(index_at)].set(high)


def setup_inputs(seed: int = 0) -> dict:
    keys = jax.random.split(jax.random.key(seed), 2)
    samples = plant(jax.random.randint(keys[0], (TOTAL, INPUTS), -8, 8), jax.random.fold_in(keys[0], 1), -8, 7).astype(jnp.int32)
    return dict(samples=samples)


def reference(samples):
    values = samples.astype(jnp.float32)
    total = values.shape[0]
    width = values.shape[1]
    padded = jnp.concatenate([values, jnp.zeros((LAGS, width), jnp.float32)], axis=0)

    def one_lag(lag):
        window = lax.dynamic_slice(padded, (lag.astype(jnp.int32), jnp.int32(0)), (total, width))
        product = jnp.dot(window.T, values, preferred_element_type=jnp.float32, precision=lax.Precision.HIGHEST)
        return product.reshape(width * width)

    lagged = lax.map(one_lag, jnp.arange(LAGS, dtype=jnp.int32))
    lagged = lagged / (16.0 * total)
    transform = jnp.fft.fft(lagged, axis=0)
    return jnp.stack([jnp.real(transform), jnp.imag(transform)]).astype(jnp.float32)
```

```python
import functools

import jax
import jax.numpy as jnp
import numpy as np
from jax import lax
from jax.experimental import pallas as pl
from jax.experimental.pallas import tpu as pltpu
from jax.sharding import PartitionSpec as P

LAGS = 128
GROUP = 8
STEP = 16


def moved(value, by):
    n = lax.axis_size("tm")
    return lax.ppermute(value, "tm", [(d, d ^ by) for d in range(n)])


def ringed(value, by):
    n = lax.axis_size("tm")
    return lax.ppermute(value, "tm", [(d, (d + by) % n) for d in range(n)])


def correlate_body(pick_ref, ext_ref, *rest, has_acc):
    acc_ref, out_ref, zeroed = rest if has_acc else (None,) + rest
    pair, span, width = ext_ref.shape
    rows = span - LAGS
    full = pair * span
    count = out_ref.shape[0]

    @pl.when(pl.program_id(0) == 0)
    def _():
        if has_acc:
            out_ref[...] = acc_ref[...]
        else:
            out_ref[...] = jnp.zeros_like(out_ref)
        zeroed[pl.ds(0, LAGS), :] = jnp.zeros((LAGS, width), jnp.bfloat16)

    for c in range(pair):
        base = LAGS + c * span
        zeroed[pl.ds(base, rows), :] = ext_ref[c, pl.ds(0, rows), :]
        zeroed[pl.ds(base + rows, LAGS), :] = jnp.zeros((LAGS, width), jnp.bfloat16)
    samples = ext_ref[...].reshape(full, width)
    picked = lax.dot_general(
        pick_ref[...], samples, (((1,), (1,)), ((), ())), preferred_element_type=jnp.float32
    )
    turned = [
        pltpu.roll(
            picked[j * STEP : (j + 1) * STEP], full - (STEP - 1), 1, stride=1, stride_axis=0
        ).astype(jnp.bfloat16)
        for j in range(count)
    ]
    shifted = jnp.concatenate(turned, axis=0)
    for m in range(0, LAGS // STEP, 2):
        right = jnp.concatenate(
            [zeroed[pl.ds(LAGS - STEP * (m + h), full), :] for h in range(2)], axis=1
        )
        product = jnp.dot(shifted, right, preferred_element_type=jnp.float32)
        for h in range(2):
            part = product[:, h * width : (h + 1) * width].reshape(count, STEP, width)
            out_ref[:, pl.ds(STEP * (m + h), STEP), :] += part


def correlate(pick, ext, acc=None):
    chunks, span, width = ext.shape
    count = pick.shape[0] // STEP
    shape = (count, LAGS, width)
    whole = pl.BlockSpec(shape, lambda i: (0, 0, 0))
    specs = [
        pl.BlockSpec(pick.shape, lambda i: (0, 0)),
        pl.BlockSpec((2, span, width), lambda i: (i, 0, 0)),
    ]
    args = [pick, ext]
    if acc is not None:
        specs.append(whole)
        args.append(acc)
    return pl.pallas_call(
        functools.partial(correlate_body, has_acc=acc is not None),
        out_shape=jax.ShapeDtypeStruct(shape, jnp.float32),
        grid=(chunks // 2,),
        in_specs=specs,
        out_specs=whole,
        scratch_shapes=[pltpu.VMEM((LAGS + 2 * span, width), jnp.bfloat16)],
        compiler_params=pltpu.CompilerParams(vmem_limit_bytes=56 << 20),
    )(*args)


def scatter_sum(partial, groups):
    n = lax.axis_size("tm")
    if groups != 4:
        peers = [[a * GROUP + p for a in range(groups)] for p in range(GROUP)]
        return lax.psum_scatter(
            partial, "tm", scatter_dimension=0, axis_index_groups=peers, tiled=False
        )
    me = lax.axis_index("tm") // GROUP
    piece = lambda k: lax.dynamic_index_in_dim(partial, (me + k) % groups, 0, keepdims=False)
    far = piece(2)
    half = far.shape[1] // 2
    up = ringed(far[:, :half], GROUP)
    down = ringed(far[:, half:], -GROUP)
    ahead, behind = piece(1), piece(3)
    ahead = jnp.concatenate([ahead[:, :half] + up, ahead[:, half:]], axis=1)
    behind = jnp.concatenate([behind[:, :half], behind[:, half:] + down], axis=1)
    return piece(0) + ringed(ahead, GROUP) + ringed(behind, -GROUP)


def transform_table(total):
    row = np.arange(LAGS)
    lag = row // STEP * STEP + STEP - 1 - row % STEP
    angle = 2.0 * np.pi / LAGS * (np.arange(LAGS)[:, None] * lag[None, :] % LAGS)
    table = np.concatenate([np.cos(angle), -np.sin(angle)], axis=0) / (16.0 * total)
    return jnp.asarray(table.astype(np.float32))


def on_device(samples):
    n = lax.axis_size("tm")
    rows, width = samples.shape
    groups = n // GROUP
    owned = width * width // n
    per = max(owned // width, 1)
    cols = min(owned, width)
    me = lax.axis_index("tm")
    place = me % GROUP
    voltages = samples.astype(jnp.bfloat16)
    edge = lax.ppermute(voltages[:LAGS], "tm", [(d, d - 1) for d in range(1, n)])
    own = jnp.concatenate([voltages, edge], axis=0)[None]

    first = (jnp.arange(groups) * GROUP + place) * owned // width
    wanted = (first[:, None] + jnp.arange(per)[None, :]).reshape(-1)
    wanted = jnp.repeat(wanted, STEP)
    pick = (wanted[:, None] == jnp.arange(width)[None, :]).astype(jnp.bfloat16)

    two, four = moved(own, 2), moved(own, 4)
    half = own.shape[1] // 2
    six = jnp.concatenate([moved(two[:, :half], 4), moved(four[:, half:], 2)], axis=1)
    near = jnp.concatenate([own, moved(own, 1)], axis=0)
    acc = correlate(pick, near)
    mid = jnp.concatenate([two, four], axis=0)
    mid = jnp.concatenate([mid, moved(mid, 1)], axis=0)
    acc = correlate(pick, mid, acc)
    far = jnp.concatenate([six, moved(six, 1)], axis=0)
    acc = correlate(pick, far, acc)

    acc = acc.reshape(groups, per, LAGS, width)
    if cols != width:
        acc = lax.dynamic_slice_in_dim(acc, me * owned % width, cols, axis=3)
    lagged = scatter_sum(acc, groups)
    lagged = jnp.concatenate([lagged[j] for j in range(per)], axis=1)
    table = transform_table(rows * n)
    out = jnp.dot(
        table, lagged, preferred_element_type=jnp.float32, precision=lax.Precision.HIGHEST
    )
    return out.reshape(2, LAGS, owned)


def solution(mesh):
    return jax.shard_map(
        on_device,
        mesh=mesh,
        in_specs=(P("tm", None),),
        out_specs=P(None, None, "tm"),
        check_vma=False,
    )
```

```python
import functools

import jax
import jax.numpy as jnp
import numpy as np
from jax import lax
from jax.experimental import pallas as pl
from jax.experimental.pallas import tpu as pltpu
from jax.sharding import PartitionSpec as P

LAGS = 128
GROUP = 8
STEP = 16


def moved(value, by):
    n = lax.axis_size("tm")
    return lax.ppermute(value, "tm", [(d, d ^ by) for d in range(n)])


def ringed(value, by):
    n = lax.axis_size("tm")
    return lax.ppermute(value, "tm", [(d, (d + by) % n) for d in range(n)])


def correlate_body(pick_ref, *rest, parts, has_acc):
    pieces, rest = rest[:parts], rest[parts:]
    acc_ref, *outs, samples, zeroed = rest if has_acc else (None,) + rest
    full, width = samples.shape
    rows = full // 2 - LAGS
    each = outs[0].shape[0]
    count = each * len(outs)

    at = 0
    for piece in pieces:
        size = piece.shape[0]
        samples[pl.ds(at, size), :] = piece[...]
        zeroed[pl.ds(LAGS + at, size), :] = piece[...]
        at += size
    blank = jnp.zeros((LAGS, width), jnp.bfloat16)
    for start in (0, LAGS + rows, 2 * (LAGS + rows)):
        zeroed[pl.ds(start, LAGS), :] = blank
    picked = lax.dot_general(
        pick_ref[...], samples[...], (((1,), (1,)), ((), ())), preferred_element_type=jnp.float32
    )
    turned = [
        pltpu.roll(
            picked[j * STEP : (j + 1) * STEP], full - (STEP - 1), 1, stride=1, stride_axis=0
        ).astype(jnp.bfloat16)
        for j in range(count)
    ]
    shifted = jnp.concatenate(turned, axis=0)
    for m in range(0, LAGS // STEP, 2):
        right = jnp.concatenate(
            [zeroed[pl.ds(LAGS - STEP * (m + h), full), :] for h in range(2)], axis=1
        )
        product = jnp.dot(shifted, right, preferred_element_type=jnp.float32)
        for h in range(2):
            part = product[:, h * width : (h + 1) * width].reshape(count, STEP, width)
            lags = pl.ds(STEP * (m + h), STEP)
            if has_acc:
                part = part + acc_ref[:, lags, :]
            for o, out_ref in enumerate(outs):
                out_ref[:, lags, :] = part[o * each : (o + 1) * each]


def correlate(pick, pieces, acc=None, share=(0, 1), outs=1):
    width = pieces[0].shape[1]
    full = sum(piece.shape[0] for piece in pieces)
    which, of = share
    count = pick.shape[0] // STEP // of
    shape = (count, LAGS, width)
    specs = [pl.BlockSpec((count * STEP, width), lambda i: (which, 0))]
    specs += [pl.BlockSpec(piece.shape, lambda i: (0, 0)) for piece in pieces]
    args = [pick, *pieces]
    if acc is not None:
        specs.append(pl.BlockSpec(shape, lambda i: (which, 0, 0)))
        args.append(acc)
    out = (count // outs, LAGS, width)
    results = pl.pallas_call(
        functools.partial(correlate_body, parts=len(pieces), has_acc=acc is not None),
        out_shape=[jax.ShapeDtypeStruct(out, jnp.float32)] * outs,
        grid=(1,),
        in_specs=specs,
        out_specs=[pl.BlockSpec(out, lambda i: (0, 0, 0))] * outs,
        scratch_shapes=[
            pltpu.VMEM((full, width), jnp.bfloat16),
            pltpu.VMEM((LAGS + full, width), jnp.bfloat16),
        ],
        compiler_params=pltpu.CompilerParams(vmem_limit_bytes=56 << 20),
    )(*args)
    return results[0] if outs == 1 else results


def ring_sum(early, rest):
    far_lo, far_hi, ahead_lo, ahead_hi = early
    up = ringed(far_lo, GROUP)
    down = ringed(far_hi, -GROUP)
    ahead_hi = ringed(ahead_hi, GROUP)
    behind_lo, behind_hi, here_lo, here_hi = rest
    ahead_lo = ringed(ahead_lo + up, GROUP)
    behind_hi = ringed(behind_hi + down, -GROUP)
    behind_lo = ringed(behind_lo, -GROUP)
    low = here_lo + behind_lo + ahead_lo
    high = here_hi + ahead_hi + behind_hi
    return [part[j] for part in (low, high) for j in range(part.shape[0])]


def scatter_sum(partial, groups):
    peers = [[a * GROUP + p for a in range(groups)] for p in range(GROUP)]
    lagged = lax.psum_scatter(
        partial, "tm", scatter_dimension=0, axis_index_groups=peers, tiled=False
    )
    return [lagged[j] for j in range(lagged.shape[0])]


def transform_table(total):
    row = np.arange(LAGS)
    lag = row // STEP * STEP + STEP - 1 - row % STEP
    angle = 2.0 * np.pi / LAGS * (np.arange(LAGS)[:, None] * lag[None, :] % LAGS)
    table = np.concatenate([np.cos(angle), -np.sin(angle)], axis=0) / (16.0 * total)
    return jnp.asarray(table.astype(np.float32))


def on_device(samples):
    n = lax.axis_size("tm")
    rows, width = samples.shape
    groups = n // GROUP
    owned = width * width // n
    per = max(owned // width, 1)
    cols = min(owned, width)
    me = lax.axis_index("tm")
    place = me % GROUP
    voltages = samples.astype(jnp.bfloat16)
    edge = lax.ppermute(voltages[:LAGS], "tm", [(d, d - 1) for d in range(1, n)])
    own = jnp.concatenate([voltages, edge], axis=0)

    ring = groups == 4 and per % 2 == 0
    order = jnp.arange(groups)
    if ring:
        order = (me // GROUP + jnp.array([2, 1, 3, 0])) % groups
    first = (order * GROUP + place) * owned // width
    wanted = (first[:, None] + jnp.arange(per)[None, :]).reshape(-1)
    wanted = jnp.repeat(wanted, STEP)
    pick = (wanted[:, None] == jnp.arange(width)[None, :]).astype(jnp.bfloat16)

    half = own.shape[0] // 2
    two, four, twin = moved(own, 2), moved(own, 4), moved(own, 1)
    acc = correlate(pick, [own, twin])
    two, four, acc = lax.optimization_barrier((two, four, acc))
    six = [moved(two[:half], 4), moved(four[half:], 2)]
    acc = correlate(pick, [two, moved(two, 1)], acc)
    acc = correlate(pick, [four, moved(four, 1)], acc)
    *six, acc = lax.optimization_barrier((*six, acc))
    six += [moved(piece, 1) for piece in six]

    if ring:
        early = correlate(pick, six, acc, (0, 2), 4)
        *early, acc = lax.optimization_barrier((*early, acc))
        late = correlate(pick, six, acc, (1, 2), 4)
        lagged = ring_sum(early, late)
    else:
        acc = correlate(pick, six, acc)
        acc = acc.reshape(groups, per, LAGS, width)
        if cols != width:
            acc = lax.dynamic_slice_in_dim(acc, me * owned % width, cols, axis=3)
        lagged = scatter_sum(acc, groups)
    lagged = jnp.concatenate(lagged, axis=1)
    table = transform_table(rows * n)
    out = jnp.dot(
        table, lagged, preferred_element_type=jnp.float32, precision=lax.Precision.HIGHEST
    )
    return out.reshape(2, LAGS, owned)


def solution(mesh):
    return jax.shard_map(
        on_device,
        mesh=mesh,
        in_specs=(P("tm", None),),
        out_specs=P(None, None, "tm"),
        check_vma=False,
    )
```

```python
import functools

import jax
import jax.numpy as jnp
import numpy as np
from jax import lax
from jax.experimental import pallas as pl
from jax.experimental.pallas import tpu as pltpu
from jax.sharding import PartitionSpec as P

LAGS = 128
GROUP = 8
STEP = 16


def moved(value, by):
    n = lax.axis_size("tm")
    return lax.ppermute(value, "tm", [(d, d ^ by) for d in range(n)])


def ringed(value, by):
    n = lax.axis_size("tm")
    return lax.ppermute(value, "tm", [(d, (d + by) % n) for d in range(n)])


def correlate_body(pick_ref, *rest, parts, has_acc, which):
    pieces, rest = rest[:parts], rest[parts:]
    acc_ref, *outs, samples, zeroed = rest if has_acc else (None,) + rest
    full, width = samples.shape
    rows = full // 2 - LAGS
    each = outs[0].shape[0]
    count = each * len(outs)

    at = 0
    for piece in pieces:
        size = piece.shape[0]
        samples[pl.ds(at, size), :] = piece[...]
        zeroed[pl.ds(LAGS + at, size), :] = piece[...]
        at += size
    blank = jnp.zeros((LAGS, width), jnp.bfloat16)
    for start in (0, LAGS + rows, 2 * (LAGS + rows)):
        zeroed[pl.ds(start, LAGS), :] = blank
    picked = lax.dot_general(
        pick_ref[pl.ds(which * count * STEP, count * STEP), :], samples[...], (((1,), (1,)), ((), ())), preferred_element_type=jnp.float32
    )
    turned = [
        pltpu.roll(
            picked[j * STEP : (j + 1) * STEP], full - (STEP - 1), 1, stride=1, stride_axis=0
        ).astype(jnp.bfloat16)
        for j in range(count)
    ]
    shifted = jnp.concatenate(turned, axis=0)
    for m in range(0, LAGS // STEP, 2):
        right = jnp.concatenate(
            [zeroed[pl.ds(LAGS - STEP * (m + h), full), :] for h in range(2)], axis=1
        )
        product = jnp.dot(shifted, right, preferred_element_type=jnp.float32)
        for h in range(2):
            part = product[:, h * width : (h + 1) * width].reshape(count, STEP, width)
            lags = pl.ds(STEP * (m + h), STEP)
            if has_acc:
                part = part + acc_ref[pl.ds(which * count, count), lags, :]
            for o, out_ref in enumerate(outs):
                out_ref[:, lags, :] = part[o * each : (o + 1) * each]


def correlate(pick, pieces, acc=None, share=(0, 1), outs=1):
    width = pieces[0].shape[1]
    full = sum(piece.shape[0] for piece in pieces)
    which, of = share
    count = pick.shape[0] // STEP // of
    args = [pick, *pieces] if acc is None else [pick, *pieces, acc]
    near = pl.BlockSpec(memory_space=pltpu.VMEM)
    out = (count // outs, LAGS, width)
    results = pl.pallas_call(
        functools.partial(correlate_body, parts=len(pieces), has_acc=acc is not None, which=which),
        out_shape=[jax.ShapeDtypeStruct(out, jnp.float32)] * outs,
        in_specs=[near] * len(args),
        out_specs=[near] * outs,
        scratch_shapes=[
            pltpu.VMEM((full, width), jnp.bfloat16),
            pltpu.VMEM((LAGS + full, width), jnp.bfloat16),
        ],
        compiler_params=pltpu.CompilerParams(vmem_limit_bytes=32 << 20),
    )(*args)
    return results[0] if outs == 1 else results


def ring_sum(early, rest):
    far_lo, far_hi, ahead_lo, ahead_hi = early
    up = ringed(far_lo, GROUP)
    down = ringed(far_hi, -GROUP)
    ahead_hi = ringed(ahead_hi, GROUP)
    behind_lo, behind_hi, here_lo, here_hi = rest
    ahead_lo = ringed(ahead_lo + up, GROUP)
    behind_hi = ringed(behind_hi + down, -GROUP)
    behind_lo = ringed(behind_lo, -GROUP)
    low = here_lo + behind_lo + ahead_lo
    high = here_hi + ahead_hi + behind_hi
    return [part[j] for part in (low, high) for j in range(part.shape[0])]


def scatter_sum(partial, groups):
    peers = [[a * GROUP + p for a in range(groups)] for p in range(GROUP)]
    lagged = lax.psum_scatter(
        partial, "tm", scatter_dimension=0, axis_index_groups=peers, tiled=False
    )
    return [lagged[j] for j in range(lagged.shape[0])]


def transform_table(total):
    row = np.arange(LAGS)
    lag = row // STEP * STEP + STEP - 1 - row % STEP
    angle = 2.0 * np.pi / LAGS * (np.arange(LAGS)[:, None] * lag[None, :] % LAGS)
    table = np.concatenate([np.cos(angle), -np.sin(angle)], axis=0) / (16.0 * total)
    return jnp.asarray(table.astype(np.float32))


def spectra_of(samples):
    n = lax.axis_size("tm")
    rows, width = samples.shape
    groups = n // GROUP
    owned = width * width // n
    per = max(owned // width, 1)
    cols = min(owned, width)
    me = lax.axis_index("tm")
    place = me % GROUP
    voltages = samples.astype(jnp.bfloat16)
    edge = lax.ppermute(voltages[:LAGS], "tm", [(d, d - 1) for d in range(1, n)])
    own = jnp.concatenate([voltages, edge], axis=0)

    ring = groups == 4 and per % 2 == 0
    order = jnp.arange(groups)
    if ring:
        order = (me // GROUP + jnp.array([2, 1, 3, 0])) % groups
    first = (order * GROUP + place) * owned // width
    wanted = (first[:, None] + jnp.arange(per)[None, :]).reshape(-1)
    wanted = jnp.repeat(wanted, STEP)
    pick = (wanted[:, None] == jnp.arange(width)[None, :]).astype(jnp.bfloat16)

    half = own.shape[0] // 2
    two, four, twin = moved(own, 2), moved(own, 4), moved(own, 1)
    acc = correlate(pick, [own, twin])
    two, four, acc = lax.optimization_barrier((two, four, acc))
    six = [moved(two[:half], 4), moved(four[half:], 2)]
    acc = correlate(pick, [two, moved(two, 1)], acc)
    acc = correlate(pick, [four, moved(four, 1)], acc)
    *six, acc = lax.optimization_barrier((*six, acc))
    six += [moved(piece, 1) for piece in six]

    if ring:
        early = correlate(pick, six, acc, (0, 2), 4)
        *early, acc = lax.optimization_barrier((*early, acc))
        late = correlate(pick, six, acc, (1, 2), 4)
        lagged = ring_sum(early, late)
    else:
        acc = correlate(pick, six, acc)
        acc = acc.reshape(groups, per, LAGS, width)
        if cols != width:
            acc = lax.dynamic_slice_in_dim(acc, me * owned % width, cols, axis=3)
        lagged = scatter_sum(acc, groups)
    lagged = jnp.concatenate(lagged, axis=1)
    table = transform_table(rows * n)
    out = jnp.dot(
        table, lagged, preferred_element_type=jnp.float32, precision=lax.Precision.HIGHEST
    )
    return out.reshape(2, LAGS, owned)


def solution(mesh):
    return jax.shard_map(
        spectra_of,
        mesh=mesh,
        in_specs=(P("tm", None),),
        out_specs=P(None, None, "tm"),
        check_vma=False,
    )
```

```python
import functools

import jax
import jax.numpy as jnp
import numpy as np
from jax import lax
from jax.experimental import pallas as pl
from jax.experimental.pallas import tpu as pltpu
from jax.sharding import PartitionSpec as P

LAGS = 128
GROUP = 8
STEP = 16


def moved(value, by):
    n = lax.axis_size("tm")
    return lax.ppermute(value, "tm", [(d, d ^ by) for d in range(n)])


def ringed(value, by):
    n = lax.axis_size("tm")
    return lax.ppermute(value, "tm", [(d, (d + by) % n) for d in range(n)])


def correlate_body(pick_ref, *rest, parts, has_acc, which):
    pieces, rest = rest[:parts], rest[parts:]
    acc_ref, *outs, samples, zeroed = rest if has_acc else (None,) + rest
    full, width = samples.shape
    rows = full // 2 - LAGS
    each = outs[0].shape[0]
    count = each * len(outs)

    at = 0
    for piece in pieces:
        size = piece.shape[0]
        samples[pl.ds(at, size), :] = piece[...]
        zeroed[pl.ds(LAGS + at, size), :] = piece[...]
        at += size
    blank = jnp.zeros((LAGS, width), jnp.bfloat16)
    for start in (0, LAGS + rows, 2 * (LAGS + rows)):
        zeroed[pl.ds(start, LAGS), :] = blank
    picked = lax.dot_general(
        pick_ref[pl.ds(which * count * STEP, count * STEP), :], samples[...], (((1,), (1,)), ((), ())), preferred_element_type=jnp.float32
    )
    turned = [
        pltpu.roll(
            picked[j * STEP : (j + 1) * STEP], full - (STEP - 1), 1, stride=1, stride_axis=0
        ).astype(jnp.bfloat16)
        for j in range(count)
    ]
    shifted = jnp.concatenate(turned, axis=0)
    for m in range(0, LAGS // STEP, 2):
        right = jnp.concatenate(
            [zeroed[pl.ds(LAGS - STEP * (m + h), full), :] for h in range(2)], axis=1
        )
        product = jnp.dot(shifted, right, preferred_element_type=jnp.float32)
        for h in range(2):
            part = product[:, h * width : (h + 1) * width].reshape(count, STEP, width)
            lags = pl.ds(STEP * (m + h), STEP)
            if has_acc:
                part = part + acc_ref[pl.ds(which * count, count), lags, :]
            for o, out_ref in enumerate(outs):
                out_ref[:, lags, :] = part[o * each : (o + 1) * each]


def correlate(pick, pieces, acc=None, share=(0, 1), outs=1):
    width = pieces[0].shape[1]
    full = sum(piece.shape[0] for piece in pieces)
    which, of = share
    count = pick.shape[0] // STEP // of
    args = [pick, *pieces] if acc is None else [pick, *pieces, acc]
    near = pl.BlockSpec(memory_space=pltpu.VMEM)
    out = (count // outs, LAGS, width)
    results = pl.pallas_call(
        functools.partial(correlate_body, parts=len(pieces), has_acc=acc is not None, which=which),
        out_shape=[jax.ShapeDtypeStruct(out, jnp.float32)] * outs,
        in_specs=[near] * len(args),
        out_specs=[near] * outs,
        scratch_shapes=[
            pltpu.VMEM((full, width), jnp.bfloat16),
            pltpu.VMEM((LAGS + full, width), jnp.bfloat16),
        ],
        compiler_params=pltpu.CompilerParams(vmem_limit_bytes=32 << 20),
    )(*args)
    return results[0] if outs == 1 else results


def ring_sum(early, rest):
    far_lo, far_hi, ahead_lo, ahead_hi = early
    up = ringed(far_lo, GROUP)
    down = ringed(far_hi, -GROUP)
    ahead_hi = ringed(ahead_hi, GROUP)
    behind_lo, behind_hi, here_lo, here_hi = rest
    ahead_lo = ringed(ahead_lo + up, GROUP)
    behind_hi = ringed(behind_hi + down, -GROUP)
    behind_lo = ringed(behind_lo, -GROUP)
    low = here_lo + behind_lo + ahead_lo
    high = here_hi + ahead_hi + behind_hi
    return [part[j] for part in (low, high) for j in range(part.shape[0])]


def scatter_sum(partial, groups):
    peers = [[a * GROUP + p for a in range(groups)] for p in range(GROUP)]
    lagged = lax.psum_scatter(
        partial, "tm", scatter_dimension=0, axis_index_groups=peers, tiled=False
    )
    return [lagged[j] for j in range(lagged.shape[0])]


def transform_table(total):
    row = np.arange(LAGS)
    lag = row // STEP * STEP + STEP - 1 - row % STEP
    angle = 2.0 * np.pi / LAGS * (np.arange(LAGS)[:, None] * lag[None, :] % LAGS)
    table = np.concatenate([np.cos(angle), -np.sin(angle)], axis=0) / (16.0 * total)
    return jnp.asarray(table.astype(np.float32))


def spectra_of(samples):
    n = lax.axis_size("tm")
    rows, width = samples.shape
    groups = n // GROUP
    owned = width * width // n
    per = max(owned // width, 1)
    cols = min(owned, width)
    me = lax.axis_index("tm")
    place = me % GROUP
    voltages = samples.astype(jnp.bfloat16)
    edge = lax.ppermute(voltages[:LAGS], "tm", [(d, d - 1) for d in range(1, n)])
    two = moved(voltages, 2)
    four = moved(voltages, 4)
    twin = moved(voltages, 1)
    edges = jnp.concatenate([edge, moved(edge, 1)], axis=0)

    ring = groups == 4 and per % 2 == 0
    order = jnp.arange(groups)
    if ring:
        order = (me // GROUP + jnp.array([2, 1, 3, 0])) % groups
    first = (order * GROUP + place) * owned // width
    wanted = (first[:, None] + jnp.arange(per)[None, :]).reshape(-1)
    wanted = jnp.repeat(wanted, STEP)
    pick = (wanted[:, None] == jnp.arange(width)[None, :]).astype(jnp.bfloat16)

    def extended(first, second, tails):
        return [*first, tails[:LAGS], *second, tails[LAGS:]]

    half = rows // 2
    acc = correlate(pick, extended([voltages], [twin], edges))
    tails = [moved(edges, by) for by in (2, 4, 6)]
    two, four, acc, *tails = lax.optimization_barrier((two, four, acc, *tails))
    six = [moved(two[:half], 4), moved(four[half:], 2)]
    acc = correlate(pick, extended([two], [moved(two, 1)], tails[0]), acc)
    acc = correlate(pick, extended([four], [moved(four, 1)], tails[1]), acc)
    *six, acc = lax.optimization_barrier((*six, acc))
    six = extended(six, [moved(piece, 1) for piece in six], tails[2])

    if ring:
        early = correlate(pick, six, acc, (0, 2), 4)
        *early, acc = lax.optimization_barrier((*early, acc))
        late = correlate(pick, six, acc, (1, 2), 4)
        lagged = ring_sum(early, late)
    else:
        acc = correlate(pick, six, acc)
        acc = acc.reshape(groups, per, LAGS, width)
        if cols != width:
            acc = lax.dynamic_slice_in_dim(acc, me * owned % width, cols, axis=3)
        lagged = scatter_sum(acc, groups)
    lagged = jnp.concatenate(lagged, axis=1)
    table = transform_table(rows * n)
    out = jnp.dot(
        table, lagged, preferred_element_type=jnp.float32, precision=lax.Precision.HIGHEST
    )
    return out.reshape(2, LAGS, owned)


def solution(mesh):
    return jax.shard_map(
        spectra_of,
        mesh=mesh,
        in_specs=(P("tm", None),),
        out_specs=P(None, None, "tm"),
        check_vma=False,
    )
```
